32 devices in a mesh: farcp: 4 (over x, core), nearcp: 4 (over z), heads: 2 (over y).
Axes of the slice: x: 2, y: 2, z: 4, core: 2. Of those that a mesh axis runs over, the one named last changes fastest.
Arguments:
- raw_keys: bfloat16 [16, 24576, 8, 128], P(None, ('farcp', 'nearcp'), 'heads'), may hold values from -6 to 6
- raw_values: bfloat16 [16, 24576, 8, 128], P(None, ('farcp', 'nearcp'), 'heads'), may hold values from -6 to 6
- turn_angle: float32 [24576, 64], replicated, may hold values from -3.140625 to 3.140625
Outputs:
- stored_keys: bfloat16 [16, 8, 128, 24576], P(('farcp', 'nearcp'), 'heads')
- stored_values: bfloat16 [16, 24576, 8, 128], P(('farcp', 'nearcp'), None, 'heads')
- page_high: bfloat16 [16, 384, 8, 128], P(('farcp', 'nearcp'), None, 'heads')
- page_low: bfloat16 [16, 384, 8, 128], P(('farcp', 'nearcp'), None, 'heads')
The draws below stay inside these ranges and needn't reach their ends.
All inputs are finite; a program needn't handle non-finite values.
Results may differ from the reference program's by a relative error of at most 0.001.
Values may be sent and summed in bfloat16 or wider, within the bound.
No kernel may reach another device: no remote copies, remote signals or barrier semaphores. Data moves between devices by JAX's collectives and lax.ppermute only.
A program may use at most 256 MiB of HBM per device.

```python
import jax
import jax.numpy as jnp

BATCH = 16
LENGTH = 24576
KV_HEADS = 8
HEAD_SIZE = 128
HALF_HEAD = 64
PAGE = 64


def shard_levels(own_key, dims, cuts, smallest, high):
    def one(dim, blocks):
        steps = jax.random.uniform(jax.random.fold_in(jax.random.fold_in(own_key, 6), dim), (blocks,), jnp.float32, smallest / len(cuts), high / len(cuts))
        return jnp.repeat(jnp.exp(steps), dims[dim] // blocks).reshape((-1,) + (1,) * (len(dims) - dim - 1))

    gain = one(*cuts[0])
    for cut in cuts[1:]:
        gain = gain * one(*cut)
    return gain


def bell_draw(rng, extent, width, reach, pieces=(), kind=jnp.bfloat16):
    gain = shard_levels(rng, extent, pieces, -0.22, 0.18) if pieces else 1.0
    array = jax.random.normal(rng, extent, jnp.float32) * width * gain
    return jnp.minimum(jnp.maximum(array, -reach), reach).astype(kind)


def setup_inputs(seed: int = 0) -> dict:
    key_of = jax.random.split(jax.random.key(seed), 4)
    return {
        "raw_keys": bell_draw(key_of[0], (BATCH, LENGTH, KV_HEADS, HEAD_SIZE), 1.0, 6.0, ((1, 16), (2, 2))),
        "raw_values": bell_draw(key_of[1], (BATCH, LENGTH, KV_HEADS, HEAD_SIZE), 1.0, 6.0, ((1, 16), (2, 2))),
        "turn_angle": jnp.clip(jax.random.uniform(key_of[2], (LENGTH, HALF_HEAD), jnp.float32, -3.140625, 3.140625), -3.140625, 3.140625),
    }


def apply_rotary(vectors, angle):
    half = vectors.shape[-1] // 2
    cosine, sine = jnp.cos(angle)[None, :, None, :], jnp.sin(angle)[None, :, None, :]
    first, second = vectors[..., :half], vectors[..., half:]
    return jnp.concatenate([first * cosine - second * sine, second * cosine + first * sine], axis=-1)


def keys_in_place(plain_keys, angle):
    wide_keys = plain_keys.astype(jnp.float32)
    return apply_rotary(wide_keys, angle)


def reference(raw_keys, raw_values, turn_angle):
    turned_keys = keys_in_place(raw_keys, turn_angle)
    narrow_keys = turned_keys.astype(jnp.bfloat16)
    page_view = narrow_keys.reshape(BATCH, LENGTH // PAGE, PAGE, KV_HEADS, HEAD_SIZE)
    page_high = jnp.max(page_view, axis=2)
    page_low = jnp.min(page_view, axis=2)
    stored_keys = jnp.transpose(narrow_keys, (0, 2, 3, 1))
    stored_values = raw_values
    return stored_keys, stored_values, page_high, page_low
```

```python
import jax
import jax.numpy as jnp
from jax import lax
from jax.sharding import PartitionSpec as P

PAGE = 64
GROUP = ("farcp", "nearcp")
SHARES = (4, 11, 1)


def apply_rotary(vectors, angle):
    half = vectors.shape[-1] // 2
    cosine, sine = (jnp.cos(angle)[None, :, None, :], jnp.sin(angle)[None, :, None, :])
    first, second = (vectors[..., :half], vectors[..., half:])
    return jnp.concatenate(
        [first * cosine - second * sine, second * cosine + first * sine], axis=-1
    )


def exchange(block):
    return lax.all_to_all(block, GROUP, split_axis=0, concat_axis=0, tiled=True)


def per_device(raw_keys, raw_values, turn_angle):
    length = raw_keys.shape[1]
    cuts = [0]
    for share in SHARES:
        cuts.append(cuts[-1] + length * share // sum(SHARES))
    parts = [raw_values[:, a:b] for a, b in zip(cuts, cuts[1:])]

    head_in, keys_in = lax.optimization_barrier((parts[0], raw_keys))
    head = exchange(head_in)

    my_angles = lax.dynamic_slice_in_dim(
        turn_angle, lax.axis_index(GROUP) * length, length
    )
    sent_keys = apply_rotary(keys_in.astype(jnp.float32), my_angles).astype(jnp.bfloat16)
    sent_keys, head = lax.optimization_barrier((sent_keys, head))
    moved_keys = exchange(sent_keys)

    body_in, moved_keys = lax.optimization_barrier((parts[1], moved_keys))
    body = exchange(body_in)
    tail_in, body = lax.optimization_barrier((parts[2], body))
    tail = exchange(tail_in)

    stored_values = jnp.zeros(raw_values.shape, raw_values.dtype)
    for start, part in zip(cuts, (head, body, tail)):
        stored_values = lax.dynamic_update_slice_in_dim(stored_values, part, start, 1)
    stored_values = stored_values.reshape((1, -1) + raw_values.shape[2:])

    moved_keys = moved_keys.reshape((1, -1) + raw_keys.shape[2:])
    page_view = moved_keys.reshape(
        moved_keys.shape[0], -1, PAGE, moved_keys.shape[2], moved_keys.shape[3]
    )
    page_high = jnp.max(page_view, axis=2)
    page_low = jnp.min(page_view, axis=2)
    stored_keys = jnp.transpose(moved_keys, (0, 2, 3, 1))
    return (stored_keys, stored_values, page_high, page_low)


def solution(mesh):
    return jax.shard_map(
        per_device,
        mesh=mesh,
        in_specs=(
            P(None, ("farcp", "nearcp"), "heads", None),
            P(None, ("farcp", "nearcp"), "heads", None),
            P(),
        ),
        out_specs=(
            P(("farcp", "nearcp"), "heads", None, None),
            P(("farcp", "nearcp"), None, "heads", None),
            P(("farcp", "nearcp"), None, "heads", None),
            P(("farcp", "nearcp"), None, "heads", None),
        ),
        check_vma=False,
    )
```
